32 devices in a mesh: gx: 4 (over x, core), gy: 8 (over z, y).
Axes of the slice: x: 2, y: 2, z: 4, core: 2. Of those that a mesh axis runs over, the one named last changes fastest.
Arguments:
- positions: float32 [32, 128, 3, 128], P('gx', 'gy'), may hold values from 0 to 1
- masses: float32 [32, 128, 128], P('gx', 'gy'), may hold values from 0.03 to 0.04
- smoothing: float32 [32, 128, 128], P('gx', 'gy'), may hold values from 0.45 to 0.5
- counts: int32 [32, 128], P('gx', 'gy'), may hold values from 64 to 128, as said below
- pair_list: int32 [32, 128, 8], P('gx', 'gy'), may hold values 0 or 1
- dest: int32 [32, 128], P('gx', 'gy'), may hold values from 0 to 4095, as said below
Outputs:
- moved_state: float32 [32, 128, 5, 128], P('gx', 'gy')
- moved_share: float32 [32, 128], P('gx', 'gy')
The draws below stay inside these ranges and needn't reach their ends.
Inputs may be any that keep to these rules, and one draw needn't show every extreme that they name: `counts`: tile slots 0 to count - 1 hold particles. `dest`: A permutation of the 4096 slots. A device's block holds slots x in [p * 8, (p + 1) * 8), y in [q * 16, (q + 1) * 16). The tiles of one device that go to one device (itself included) number 0 or exactly 8.
All inputs are finite; a program needn't handle non-finite values. No bound on the sum of `pair_list` on one device may be relied on, other than what follows from the above.
Results may differ from the reference program's by a relative error of at most 0.0003.
Values sent between devices are 32-bit elements; how exact they have to be, the bound alone decides.
A program may use at most 64 MiB of HBM per device.

```python
import math
import jax
import jax.numpy as jnp
from jax import lax

TILE = 128
CX = 8
CY = 16
CAP = 8
TX = 32
TY = 128


def draw_counts(key, part):
    row_ids = jnp.arange(TX, dtype=jnp.int32)
    ceiling = 72 + 56 * row_ids // max(TX - 1, 1)
    raw_bits = jax.random.randint(key, (TX, TY), 0, 1 << 20, dtype=jnp.int32)
    counts = ceiling[:, None] - raw_bits % 9
    counts = counts.at[0, 0].set(64)
    return counts.at[TX - 1, 0].set(128).astype(jnp.int32)


def shuffled(subkey, length):
    return jax.random.permutation(subkey, length).astype(jnp.int32)


def draw_dest(key, part):
    grid_x = TX // CX
    grid_y = TY // CY
    device_total = grid_x * grid_y
    tile_total = CX * CY
    blocks = tile_total // CAP
    keys = jax.random.split(jax.random.fold_in(key, 7), 4)
    relabel = shuffled(keys[0], device_total)
    inverse = jnp.zeros((device_total,), jnp.int32).at[relabel].set(jnp.arange(device_total, dtype=jnp.int32))
    shifts = shuffled(keys[1], device_total)[:blocks]
    source_order = jax.vmap(lambda subkey: shuffled(subkey, tile_total))(jax.random.split(keys[2], device_total))
    slot_order = jax.vmap(lambda subkey: shuffled(subkey, tile_total))(jax.random.split(keys[3], device_total))
    row_ids = jnp.arange(TX, dtype=jnp.int32)[:, None]
    col_ids = jnp.arange(TY, dtype=jnp.int32)[None, :]
    source = row_ids // CX * grid_y + col_ids // CY
    local = row_ids % CX * CY + col_ids % CY
    position = source_order[source, local]
    block = position // CAP
    target = inverse[(relabel[source] + shifts[block]) % device_total]
    slot_local = slot_order[target, position]
    slot_x = target // grid_y * CX + slot_local // CY
    slot_y = target % grid_y * CY + slot_local % CY
    return (slot_x * TY + slot_y).astype(jnp.int32)


def touch_ends(result, own_key, low, high):
    extent = result.shape
    place = [jax.random.randint(jax.random.fold_in(own_key, axis), (), 0, extent[axis]) for axis in range(len(extent))]
    result = result.at[tuple(place)].set(low)
    longest = extent.index(max(extent))
    place[longest] = (place[longest] + 1) % extent[longest]
    return result.at[tuple(place)].set(high)


def block_scale(stream_key, extent, pieces, low, largest):
    def one(dim, blocks):
        heights = jax.random.uniform(jax.random.fold_in(jax.random.fold_in(stream_key, 6), dim), (blocks,), jnp.float32, low / len(pieces), largest / len(pieces))
        return jnp.repeat(jnp.exp(heights), extent[dim] // blocks).reshape((-1,) + (1,) * (len(extent) - dim - 1))

    gain = one(*pieces[0])
    for cut in pieces[1:]:
        gain = gain * one(*cut)
    return gain


def setup_inputs(seed: int = 0) -> dict:
    key_list = jax.random.split(jax.random.key(seed), 7)
    return {
        "positions": jnp.clip(1.0 * jax.random.uniform(key_list[0], (TX, TY, 3, TILE), jnp.float32) ** block_scale(key_list[0], (TX, TY, 3, TILE), ((0, 4), (1, 8)), -0.2, 0.2), 0.0, 1.0),
        "masses": jnp.clip(jnp.exp(math.log(0.04) - 0.2876821 * jax.random.uniform(key_list[1], (TX, TY, TILE), jnp.float32) ** block_scale(key_list[1], (TX, TY, TILE), ((0, 4), (1, 8)), -0.2, 0.2)), 0.03, 0.04),
        "smoothing": jnp.clip(jnp.exp(math.log(0.5) - 0.105360542 * jax.random.uniform(key_list[2], (TX, TY, TILE), jnp.float32) ** block_scale(key_list[2], (TX, TY, TILE), ((0, 4), (1, 8)), -0.2, 0.2)), 0.45, 0.5),
        "counts": draw_counts(jax.random.fold_in(key_list[6], 71), 0),
        "pair_list": touch_ends((jax.random.randint(key_list[4], (TX, TY, 8), 0, 4) < 3).astype(jnp.int32), jax.random.fold_in(key_list[4], 1), 0, 1),
        "dest": draw_dest(jax.random.fold_in(key_list[6], 71), 0),
    }


def spline(ratio):
    inner_part = 1.0 - 1.5 * ratio * ratio + 0.75 * ratio * ratio * ratio
    remain = jnp.maximum(2.0 - ratio, 0.0)
    outer_part = 0.25 * remain * remain * remain
    return jnp.where(ratio < 1.0, inner_part, outer_part)

def tile_density(pos_self, smooth_self, pos_other, mass_other, step_x, step_y):
    offset = jnp.array([step_x, step_y, 0.0], dtype=jnp.float32)
    delta = pos_other[:, :, None, :] + offset[None, :, None, None] - pos_self[:, :, :, None]
    dist_sq = lax.optimization_barrier(jnp.sum(delta * delta, axis=1))
    ratio = jnp.sqrt(dist_sq) / smooth_self[:, :, None]
    kernel = spline(ratio) * mass_other[:, None, :]
    return lax.optimization_barrier(jnp.sum(kernel, axis=2)) / (math.pi * smooth_self * smooth_self * smooth_self)

def reference(positions, masses, smoothing, counts, pair_list, dest):
    slot_ids = jnp.arange(TILE, dtype=jnp.int32)
    valid_slot = slot_ids[None, None, :] < counts[:, :, None]
    masked = jnp.where(valid_slot, masses, jnp.zeros_like(masses))
    weights = pair_list.astype(jnp.float32)

    def row_density(row_index):
        pos_self = lax.dynamic_index_in_dim(positions, row_index, 0, keepdims=False)
        smooth_self = lax.dynamic_index_in_dim(smoothing, row_index, 0, keepdims=False)
        weight_row = lax.dynamic_index_in_dim(weights, row_index, 0, keepdims=False)
        summed = jnp.zeros((TY, TILE), jnp.float32)
        offset_index = 0
        for step_x in (-1, 0, 1):
            other_row = ((row_index + step_x) % TX).astype(jnp.int32)
            pos_row = lax.dynamic_index_in_dim(positions, other_row, 0, keepdims=False)
            mass_row = lax.dynamic_index_in_dim(masked, other_row, 0, keepdims=False)
            for step_y in (-1, 0, 1):
                pos_other = jnp.roll(pos_row, -step_y, axis=0)
                mass_other = jnp.roll(mass_row, -step_y, axis=0)
                contrib = tile_density(pos_self, smooth_self, pos_other, mass_other, step_x, step_y)
                if step_x == 0 and step_y == 0:
                    summed = summed + contrib
                else:
                    summed = summed + weight_row[:, offset_index][:, None] * contrib
                    offset_index += 1
        return summed
    density = lax.map(row_density, jnp.arange(TX, dtype=jnp.int32))
    density = jnp.where(valid_slot, density, jnp.zeros_like(density))
    tile_count = counts.astype(jnp.float32)
    neighbour_sum = jnp.zeros((TX, TY), jnp.float32)
    offset_index = 0
    for step_x in (-1, 0, 1):
        for step_y in (-1, 0, 1):
            if step_x == 0 and step_y == 0:
                continue
            rolled = jnp.roll(tile_count, (-step_x, -step_y), (0, 1))
            neighbour_sum = neighbour_sum + weights[:, :, offset_index] * rolled
            offset_index += 1
    pair_work = tile_count * (tile_count + neighbour_sum)
    total_work = jnp.sum(pair_work)
    work_share = pair_work * (TX * TY) / total_work
    tile_state = jnp.concatenate([positions, masked[:, :, None, :], density[:, :, None, :]], axis=2)
    flat_dest = dest.reshape(-1)
    moved_state = jnp.zeros((TX * TY, 5, TILE), jnp.float32).at[flat_dest].set(tile_state.reshape(TX * TY, 5, TILE))
    moved_share = jnp.zeros((TX * TY,), jnp.float32).at[flat_dest].set(work_share.reshape(-1))
    return (moved_state.reshape(TX, TY, 5, TILE), moved_share.reshape(TX, TY))
```

```python
import functools
import math

import jax
import jax.numpy as jnp
from jax import lax
from jax.experimental import pallas as pl
from jax.experimental.pallas import tpu as pltpu
from jax.sharding import PartitionSpec as P

OFFSETS = tuple((a, b) for a in (-1, 0, 1) for b in (-1, 0, 1) if (a, b) != (0, 0))
UNROLL = 4


def extended(block, sides, width):
    for axis, dim in sides:
        count = lax.axis_size(axis)
        forward = [(i, i + 1) for i in range(count - 1)]
        forward.append((count - 1, 0))
        backward = [(target, source) for source, target in forward]
        low = lax.ppermute(
            lax.slice_in_dim(block, block.shape[dim] - width, None, axis=dim), axis, forward
        )
        high = lax.ppermute(lax.slice_in_dim(block, 0, width, axis=dim), axis, backward)
        block = jnp.concatenate([low, block, high], axis=dim)
    return block


def list_kernel(rows, cols, pair_ref, list_ref, count_ref):
    wide = cols + 2
    dummy = (rows + 2) * wide

    def tile(t, ptr):
        tx, ty = t // cols, lax.rem(t, cols)
        base = (tx + 1) * wide + ty + 1
        list_ref[ptr] = (base << 16) | (t << 4) | 4
        ptr = ptr + 1
        for k, (a, b) in enumerate(OFFSETS):
            code = (a + 1) * 3 + (b + 1)
            list_ref[ptr] = ((base + a * wide + b) << 16) | (t << 4) | code
            ptr = ptr + jnp.where(pair_ref[t * 8 + k] != 0, 1, 0)
        return ptr

    ptr = lax.fori_loop(0, rows * cols, tile, jnp.int32(0))
    for u in range(UNROLL):
        list_ref[ptr + u] = dummy << 16
    count_ref[0] = (ptr + UNROLL - 1) // UNROLL


def split3(value):
    high = value.astype(jnp.bfloat16).astype(jnp.float32)
    rest = value - high
    mid = rest.astype(jnp.bfloat16).astype(jnp.float32)
    return high, mid, rest - mid


def density_kernel(
    tiles, sources, list_ref, count_ref, send_ref, feat_ref, own_ref, norm_ref,
    out_ref, lhs_ref, mass_ref, acc_ref
):
    width = norm_ref.shape[1]

    def prep(s, carry):
        feat = feat_ref[s]
        high, mid, low = split3(feat)
        block = jnp.concatenate([high, high, mid, mid, high, low, feat], axis=0)
        turned = block.T
        lhs_ref[s] = turned[:, :48].astype(jnp.bfloat16)
        mass_ref[s] = jnp.broadcast_to(turned[:, 53:54], (width, width))
        return carry

    lax.fori_loop(0, sources, prep, 0, unroll=2)
    lhs_ref[sources] = jnp.zeros((width, 48), jnp.bfloat16)
    mass_ref[sources] = jnp.zeros((width, width), jnp.float32)
    acc_ref[...] = jnp.zeros_like(acc_ref)
    out_ref[...] = jnp.zeros_like(out_ref)

    def step(i, carry):
        parts = []
        for u in range(UNROLL):
            entry = list_ref[i * UNROLL + u]
            source = entry >> 16
            t = (entry >> 4) & 4095
            code = entry & 15
            a = code // 3 - 1
            b = lax.rem(code, 3) - 1
            off_x = a.astype(jnp.float32)
            off_y = b.astype(jnp.float32)
            off_sq = (a * a + b * b).astype(jnp.float32)
            own = own_ref[t]
            form = own[0:8] + off_x * own[8:16] + off_y * own[16:24] + off_sq * own[24:32]
            high, mid, low = split3(form)
            rhs = jnp.concatenate([high, mid, high, mid, low, high], axis=0).astype(jnp.bfloat16)
            sq = jnp.dot(lhs_ref[source], rhs, preferred_element_type=jnp.float32)
            sq = jnp.maximum(sq, 1e-20)
            ratio = sq * lax.rsqrt(sq)
            outer = jnp.maximum(2.0 - ratio, 0.0)
            inner = jnp.maximum(1.0 - ratio, 0.0)
            value = (outer * outer * outer - 4.0 * (inner * inner * inner)) * mass_ref[source]
            parts.append((t, jnp.sum(value.reshape(width // 8, 8, width), axis=0)))
        for t, part in parts:
            acc_ref[t] += part
        return carry

    lax.fori_loop(0, count_ref[0], step, 0)

    def finish(t, carry):
        total = jnp.sum(acc_ref[t], axis=0, keepdims=True)
        out_ref[pl.ds(send_ref[t], 1), :] = total * norm_ref[pl.ds(t, 1), :]
        return carry

    lax.fori_loop(0, tiles, finish, 0, unroll=4)


def place_kernel(tiles, from_ref, state_ref, dens_ref, out_ref):
    def put(s, carry):
        row = from_ref[s]
        out_ref[s, 0:4, :] = state_ref[row, 0:4, :]
        out_ref[s, 4:5, :] = dens_ref[pl.ds(row, 1), :]
        return carry

    lax.fori_loop(0, tiles, put, 0, unroll=8)


SMEM = pl.BlockSpec(memory_space=pltpu.SMEM)
VMEM = pl.BlockSpec(memory_space=pltpu.VMEM)


def body(positions, masses, smoothing, counts, pair_list, dest):
    rows_local, cols_local = counts.shape
    slot_width = masses.shape[2]
    grid_x = lax.axis_size("gx")
    grid_y = lax.axis_size("gy")
    device_total = grid_x * grid_y
    tile_total = rows_local * cols_local
    capacity = max(2, 2 * tile_total // device_total)
    send_rows = device_total * capacity
    slot_ids = jnp.arange(slot_width, dtype=jnp.int32)
    valid_slot = slot_ids[None, None, :] < counts[:, :, None]
    masked = jnp.where(valid_slot, masses, jnp.zeros_like(masses))
    packed = jnp.concatenate([positions, masked[:, :, None, :]], axis=2)
    padded = extended(packed, (("gx", 0), ("gy", 1)), 1)
    weights = pair_list.astype(jnp.float32)

    list_size = 9 * tile_total + 2 * UNROLL
    pair_entries, pair_groups = pl.pallas_call(
        functools.partial(list_kernel, rows_local, cols_local),
        out_shape=(
            jax.ShapeDtypeStruct((list_size,), jnp.int32),
            jax.ShapeDtypeStruct((1,), jnp.int32),
        ),
        in_specs=[SMEM],
        out_specs=(SMEM, SMEM),
        cost_estimate=pl.CostEstimate(flops=4000000, bytes_accessed=8192, transcendentals=0),
        name="pair_entries",
    )(pair_list.reshape(-1))

    centred = (positions - 0.5).reshape(tile_total, 3, slot_width)
    smooth = smoothing.reshape(tile_total, 1, slot_width)
    inv_sq = 1.0 / (smooth * smooth)
    own_x, own_y, own_z = centred[:, 0:1], centred[:, 1:2], centred[:, 2:3]
    own_sq = own_x * own_x + own_y * own_y + own_z * own_z
    zero = jnp.zeros_like(inv_sq)
    own_form = jnp.concatenate(
        [-2.0 * inv_sq * own_x, -2.0 * inv_sq * own_y, -2.0 * inv_sq * own_z, inv_sq, inv_sq * own_sq,
         zero, zero, zero,
         2.0 * inv_sq, zero, zero, zero, -2.0 * inv_sq * own_x, zero, zero, zero,
         zero, 2.0 * inv_sq, zero, zero, -2.0 * inv_sq * own_y, zero, zero, zero,
         zero, zero, zero, zero, inv_sq, zero, zero, zero],
        axis=1,
    )
    norm = jnp.where(valid_slot, 0.25 / (math.pi * smoothing * smoothing * smoothing), 0.0)
    norm = norm.reshape(tile_total, slot_width)

    row_span = cols_local * grid_y
    slot_x = dest // row_span
    slot_y = dest % row_span
    target = (slot_x // rows_local * grid_y + slot_y // cols_local).reshape(-1)
    slot_local = (slot_x % rows_local * cols_local + slot_y % cols_local).reshape(-1)
    tile_order = jnp.arange(tile_total, dtype=jnp.int32)
    same_target = target[:, None] == target[None, :]
    earlier = tile_order[None, :] < tile_order[:, None]
    rank_slot = jnp.sum(jnp.logical_and(same_target, earlier).astype(jnp.int32), axis=1)
    send_index = target * capacity + rank_slot

    tile_count = counts.astype(jnp.float32)
    padded_count = jnp.sum((padded[:, :, 3, :] > 0.0).astype(jnp.float32), axis=-1)
    neighbour_sum = jnp.zeros((rows_local, cols_local), jnp.float32)
    for k, (a, b) in enumerate(OFFSETS):
        beside = padded_count[1 + a : 1 + a + rows_local, 1 + b : 1 + b + cols_local]
        neighbour_sum = neighbour_sum + weights[:, :, k] * beside
    pair_work = tile_count * (tile_count + neighbour_sum)
    local_work = jnp.sum(pair_work)

    lane = slot_ids[None, :]
    note = jnp.where(lane == 0, pair_work.reshape(-1, 1), 0.0)
    note = jnp.where(lane == 1, (slot_local + 1).astype(jnp.float32)[:, None], note)
    tile_state = jnp.concatenate(
        [packed.reshape(tile_total, 4, slot_width), note[:, None, :]], axis=1
    )
    send_state = jnp.zeros((send_rows, 5, slot_width), jnp.float32).at[send_index].set(tile_state)
    mark = jnp.logical_and(jnp.arange(5)[:, None] == 4, lane == 2)
    send_state = jnp.where(mark[None], local_work, send_state)
    recv_state = lax.all_to_all(
        send_state.reshape(device_total, capacity, 5, slot_width),
        ("gx", "gy"),
        split_axis=0,
        concat_axis=0,
        tiled=True,
    ).reshape(send_rows, 5, slot_width)

    sources = (rows_local + 2) * (cols_local + 2)
    halo = padded.reshape(sources, 4, slot_width)
    halo_pos = halo[:, :3] - 0.5
    halo_sq = jnp.sum(halo_pos * halo_pos, axis=1, keepdims=True)
    halo_one = jnp.ones_like(halo_sq)
    features = jnp.concatenate(
        [halo_pos, halo_sq, halo_one, halo[:, 3:4], 0.0 * halo_one, 0.0 * halo_one], axis=1
    )
    send_density = pl.pallas_call(
        functools.partial(density_kernel, tile_total, sources),
        out_shape=jax.ShapeDtypeStruct((send_rows, slot_width), jnp.float32),
        in_specs=[SMEM, SMEM, SMEM, VMEM, VMEM, VMEM],
        out_specs=VMEM,
        scratch_shapes=[
            pltpu.VMEM((sources + 1, slot_width, 48), jnp.bfloat16),
            pltpu.VMEM((sources + 1, slot_width, slot_width), jnp.float32),
            pltpu.VMEM((tile_total, 8, slot_width), jnp.float32),
        ],
        compiler_params=pltpu.CompilerParams(vmem_limit_bytes=40 * 1024 * 1024),
        cost_estimate=pl.CostEstimate(
            flops=20 * 9 * tile_total * slot_width * slot_width,
            bytes_accessed=180 * 2**20,
            transcendentals=9 * tile_total * slot_width * slot_width,
        ),
        name="density",
    )(pair_entries, pair_groups, send_index, features, own_form, norm)

    recv_density = lax.all_to_all(
        send_density.reshape(device_total, capacity, slot_width),
        ("gx", "gy"),
        split_axis=0,
        concat_axis=0,
        tiled=True,
    ).reshape(send_rows, slot_width)

    recv_note = recv_state[:, 4, :3]
    recv_slot = recv_note[:, 1].astype(jnp.int32) - 1
    hit = recv_slot[None, :] == tile_order[:, None]
    recv_order = jnp.arange(send_rows, dtype=jnp.int32)
    from_row = jnp.sum(jnp.where(hit, recv_order[None, :], 0), axis=1)
    total_work = jnp.sum(recv_note.reshape(device_total, capacity, 3)[:, 0, 2])
    moved_work = jnp.sum(jnp.where(hit, recv_note[:, 0][None, :], 0.0), axis=1)
    moved_share = moved_work * float(tile_total * device_total) / total_work

    moved_state = pl.pallas_call(
        functools.partial(place_kernel, tile_total),
        out_shape=jax.ShapeDtypeStruct((tile_total, 5, slot_width), jnp.float32),
        in_specs=[SMEM, VMEM, VMEM],
        out_specs=VMEM,
        name="place",
    )(from_row, recv_state, recv_density)
    return (
        moved_state.reshape(rows_local, cols_local, 5, slot_width),
        moved_share.reshape(rows_local, cols_local),
    )


def solution(mesh):
    in_specs = (
        P("gx", "gy", None, None),
        P("gx", "gy", None),
        P("gx", "gy", None),
        P("gx", "gy"),
        P("gx", "gy", None),
        P("gx", "gy"),
    )
    out_specs = (P("gx", "gy", None, None), P("gx", "gy"))
    return jax.shard_map(body, mesh=mesh, in_specs=in_specs, out_specs=out_specs, check_vma=False)
```

```python
import functools
import math

import jax
import jax.numpy as jnp
from jax import lax
from jax.experimental import pallas as pl
from jax.experimental.pallas import tpu as pltpu
from jax.sharding import PartitionSpec as P

OFFSETS = tuple((a, b) for a in (-1, 0, 1) for b in (-1, 0, 1) if (a, b) != (0, 0))
UNROLL = 4


def extended(block, sides, width):
    for axis, dim in sides:
        count = lax.axis_size(axis)
        forward = [(i, i + 1) for i in range(count - 1)]
        forward.append((count - 1, 0))
        backward = [(target, source) for source, target in forward]
        low = lax.ppermute(
            lax.slice_in_dim(block, block.shape[dim] - width, None, axis=dim), axis, forward
        )
        high = lax.ppermute(lax.slice_in_dim(block, 0, width, axis=dim), axis, backward)
        block = jnp.concatenate([low, block, high], axis=dim)
    return block


def split3(value):
    high = value.astype(jnp.bfloat16).astype(jnp.float32)
    rest = value - high
    mid = rest.astype(jnp.bfloat16).astype(jnp.float32)
    return high, mid, rest - mid


def density_kernel(
    rows, cols, pair_ref, send_ref, halo_ref, smooth_ref,
    out_ref, lhs_ref, mass_ref, own_ref, sq_ref, acc_ref, list_ref
):
    tiles = rows * cols
    width = smooth_ref.shape[1]
    wide = cols + 2
    sources = (rows + 2) * wide
    row = lax.broadcasted_iota(jnp.int32, (8, width), 0)

    def spread(ref, tile, index):
        return jnp.broadcast_to(ref[tile, index : index + 1, :], (8, width))

    def centre(t):
        tx = t // cols
        return (tx + 1) * wide + (t - tx * cols) + 1

    def point(tile):
        x = spread(halo_ref, tile, 0) - 0.5
        y = spread(halo_ref, tile, 1) - 0.5
        z = spread(halo_ref, tile, 2) - 0.5
        return x, y, z, x * x + y * y + z * z

    def prep(s, ptr):
        x, y, z, norm_sq = point(s)
        root = spread(halo_ref, s, 3)
        feat = jnp.where(row == 0, x, jnp.where(row == 1, y, jnp.where(row == 2, z, 0.0)))
        feat = jnp.where(row == 3, norm_sq, jnp.where(row == 4, 1.0, feat)) * (root * root)
        high, mid, low = split3(feat)
        turned = jnp.concatenate([high, high, mid, mid, high, low, root], axis=0).T
        lhs_ref[s] = turned[:, :48].astype(jnp.bfloat16)
        mass = jnp.broadcast_to(turned[:, 48:49], (width, width))
        mass_ref[s, 0] = mass
        mass_ref[s, 1] = mass + mass

        t = jnp.minimum(s, tiles - 1)
        base = centre(t)
        x, y, z, norm_sq = point(base)
        h = jnp.broadcast_to(smooth_ref[pl.ds(t, 1), :], (8, width))
        inv = 1.0 / (h * h)
        plain = jnp.where(row == 0, x, jnp.where(row == 1, y, z)) * -2.0
        plain = jnp.where(row < 3, plain, jnp.where(row == 3, 1.0, norm_sq))
        own_ref[t, 0] = jnp.where(row < 5, plain * inv, 0.0)
        own_ref[t, 1] = jnp.where(row == 0, 2.0, jnp.where(row == 4, -2.0 * x, 0.0)) * inv
        own_ref[t, 2] = jnp.where(row == 1, 2.0, jnp.where(row == 4, -2.0 * y, 0.0)) * inv
        own_ref[t, 3] = jnp.where(row == 4, inv, 0.0)
        live = jnp.where(s < tiles, 1, 0)
        list_ref[ptr] = (base << 16) | (t << 4) | 5
        ptr = ptr + live
        for k, (a, b) in enumerate(OFFSETS):
            code = (a + 1) * 4 + (b + 1)
            list_ref[ptr] = ((base + a * wide + b) << 16) | (t << 4) | code
            ptr = ptr + jnp.where(pair_ref[t * 8 + k] != 0, live, 0)
        return ptr

    total = lax.fori_loop(0, sources, prep, jnp.int32(0))
    for u in range(3 * UNROLL):
        list_ref[total + u] = (sources << 16) | 5
    lhs_ref[sources] = jnp.zeros((width, 48), jnp.bfloat16)
    mass_ref[sources] = jnp.zeros((2, width, width), jnp.float32)
    acc_ref[...] = jnp.zeros_like(acc_ref)
    out_ref[...] = jnp.zeros_like(out_ref)

    def products(first, slot):
        for u in range(UNROLL):
            entry = list_ref[first + u]
            t = (entry >> 4) & 4095
            off_x = (((entry >> 2) & 3) - 1).astype(jnp.float32)
            off_y = ((entry & 3) - 1).astype(jnp.float32)
            off_sq = off_x * off_x + off_y * off_y
            form = own_ref[t, 0] + off_x * own_ref[t, 1] + off_y * own_ref[t, 2] + off_sq * own_ref[t, 3]
            high, mid, low = split3(form)
            rhs = jnp.concatenate([high, mid, high, mid, low, high], axis=0).astype(jnp.bfloat16)
            sq_ref[slot, u] = jnp.dot(
                lhs_ref[entry >> 16], rhs, preferred_element_type=jnp.float32
            )

    def sums(first, slot):
        for u in range(UNROLL):
            entry = list_ref[first + u]
            source = entry >> 16
            t = (entry >> 4) & 4095
            outer_sum = jnp.zeros((8, width), jnp.float32)
            inner_sum = jnp.zeros((8, width), jnp.float32)
            for g in range(width // 8):
                at = pl.ds(8 * g, 8)
                sq = jnp.maximum(sq_ref[slot, u, at, :], 1e-20)
                ratio = sq * lax.rsqrt(sq)
                outer = jnp.maximum(mass_ref[source, 1, at, :] - ratio, 0.0)
                inner = jnp.maximum(mass_ref[source, 0, at, :] - ratio, 0.0)
                outer_sum = outer_sum + outer * outer * outer
                inner_sum = inner_sum + inner * inner * inner
            acc_ref[t] += outer_sum - 4.0 * inner_sum

    products(0, 0)

    def step(i, carry):
        first = i * (2 * UNROLL)
        products(first + UNROLL, 1)
        sums(first, 0)
        products(first + 2 * UNROLL, 0)
        sums(first + UNROLL, 1)
        return carry

    lax.fori_loop(0, (total + 2 * UNROLL - 1) // (2 * UNROLL), step, 0)

    def finish(t, carry):
        summed = jnp.sum(acc_ref[t], axis=0, keepdims=True)
        h = smooth_ref[pl.ds(t, 1), :]
        norm = 0.25 / (math.pi * h * h * h)
        alive = halo_ref[centre(t), 3:4, :] > 0.0
        out_ref[pl.ds(send_ref[t], 1), :] = jnp.where(alive, summed * norm, 0.0)
        return carry

    lax.fori_loop(0, tiles, finish, 0, unroll=4)


def place_kernel(tiles, from_ref, state_ref, dens_ref, out_ref):
    def put(s, carry):
        row = from_ref[s]
        out_ref[s, 0:4, :] = state_ref[row, 0:4, :]
        out_ref[s, 4:5, :] = dens_ref[pl.ds(row, 1), :]
        return carry

    lax.fori_loop(0, tiles, put, 0, unroll=8)


SMEM = pl.BlockSpec(memory_space=pltpu.SMEM)
VMEM = pl.BlockSpec(memory_space=pltpu.VMEM)


def body(positions, masses, smoothing, counts, pair_list, dest):
    rows_local, cols_local = counts.shape
    slot_width = masses.shape[2]
    grid_x = lax.axis_size("gx")
    grid_y = lax.axis_size("gy")
    device_total = grid_x * grid_y
    tile_total = rows_local * cols_local
    capacity = max(2, 2 * tile_total // device_total)
    send_rows = device_total * capacity
    slot_ids = jnp.arange(slot_width, dtype=jnp.int32)
    valid_slot = slot_ids[None, None, :] < counts[:, :, None]
    masked = jnp.where(valid_slot, masses, jnp.zeros_like(masses))
    packed = jnp.concatenate([positions, masked[:, :, None, :]], axis=2)
    root = jnp.where(valid_slot, jnp.cbrt(masses), jnp.zeros_like(masses))
    rooted = jnp.concatenate([positions, root[:, :, None, :]], axis=2)
    padded = extended(rooted, (("gx", 0), ("gy", 1)), 1)
    weights = pair_list.astype(jnp.float32)

    row_span = cols_local * grid_y
    slot_x = dest // row_span
    slot_y = dest % row_span
    target = (slot_x // rows_local * grid_y + slot_y // cols_local).reshape(-1)
    slot_local = (slot_x % rows_local * cols_local + slot_y % cols_local).reshape(-1)
    tile_order = jnp.arange(tile_total, dtype=jnp.int32)
    same_target = target[:, None] == target[None, :]
    earlier = tile_order[None, :] < tile_order[:, None]
    rank_slot = jnp.sum(jnp.logical_and(same_target, earlier).astype(jnp.int32), axis=1)
    send_index = target * capacity + rank_slot

    tile_count = counts.astype(jnp.float32)
    padded_count = jnp.sum((padded[:, :, 3, :] > 0.0).astype(jnp.float32), axis=-1)
    neighbour_sum = jnp.zeros((rows_local, cols_local), jnp.float32)
    for k, (a, b) in enumerate(OFFSETS):
        beside = padded_count[1 + a : 1 + a + rows_local, 1 + b : 1 + b + cols_local]
        neighbour_sum = neighbour_sum + weights[:, :, k] * beside
    pair_work = tile_count * (tile_count + neighbour_sum)
    local_work = jnp.sum(pair_work)

    lane = slot_ids[None, :]
    note = jnp.where(lane == 0, pair_work.reshape(-1, 1), 0.0)
    note = jnp.where(lane == 1, (slot_local + 1).astype(jnp.float32)[:, None], note)
    tile_state = jnp.concatenate(
        [packed.reshape(tile_total, 4, slot_width), note[:, None, :]], axis=1
    )
    send_state = jnp.zeros((send_rows, 5, slot_width), jnp.float32).at[send_index].set(tile_state)
    mark = jnp.logical_and(jnp.arange(5)[:, None] == 4, lane == 2)
    send_state = jnp.where(mark[None], local_work, send_state)
    recv_state = lax.all_to_all(
        send_state.reshape(device_total, capacity, 5, slot_width),
        ("gx", "gy"),
        split_axis=0,
        concat_axis=0,
        tiled=True,
    ).reshape(send_rows, 5, slot_width)

    sources = (rows_local + 2) * (cols_local + 2)
    send_density = pl.pallas_call(
        functools.partial(density_kernel, rows_local, cols_local),
        out_shape=jax.ShapeDtypeStruct((send_rows, slot_width), jnp.float32),
        in_specs=[SMEM, SMEM, VMEM, VMEM],
        out_specs=VMEM,
        scratch_shapes=[
            pltpu.VMEM((sources + 1, slot_width, 48), jnp.bfloat16),
            pltpu.VMEM((sources + 1, 2, slot_width, slot_width), jnp.float32),
            pltpu.VMEM((tile_total, 4, 8, slot_width), jnp.float32),
            pltpu.VMEM((2, UNROLL, slot_width, slot_width), jnp.float32),
            pltpu.VMEM((tile_total, 8, slot_width), jnp.float32),
            pltpu.SMEM((9 * tile_total + 4 * UNROLL,), jnp.int32),
        ],
        compiler_params=pltpu.CompilerParams(vmem_limit_bytes=52 * 1024 * 1024),
        cost_estimate=pl.CostEstimate(
            flops=20 * 9 * tile_total * slot_width * slot_width,
            bytes_accessed=180 * 2**20,
            transcendentals=9 * tile_total * slot_width * slot_width,
        ),
        name="density",
    )(
        pair_list.reshape(-1),
        send_index,
        padded.reshape(sources, 4, slot_width),
        smoothing.reshape(tile_total, slot_width),
    )

    recv_density = lax.all_to_all(
        send_density.reshape(device_total, capacity, slot_width),
        ("gx", "gy"),
        split_axis=0,
        concat_axis=0,
        tiled=True,
    ).reshape(send_rows, slot_width)

    recv_note = recv_state[:, 4, :3]
    recv_slot = recv_note[:, 1].astype(jnp.int32) - 1
    hit = recv_slot[None, :] == tile_order[:, None]
    recv_order = jnp.arange(send_rows, dtype=jnp.int32)
    from_row = jnp.sum(jnp.where(hit, recv_order[None, :], 0), axis=1)
    total_work = jnp.sum(recv_note.reshape(device_total, capacity, 3)[:, 0, 2])
    moved_work = jnp.sum(jnp.where(hit, recv_note[:, 0][None, :], 0.0), axis=1)
    moved_share = moved_work * float(tile_total * device_total) / total_work

    moved_state = pl.pallas_call(
        functools.partial(place_kernel, tile_total),
        out_shape=jax.ShapeDtypeStruct((tile_total, 5, slot_width), jnp.float32),
        in_specs=[SMEM, VMEM, VMEM],
        out_specs=VMEM,
        name="place",
    )(from_row, recv_state, recv_density)
    return (
        moved_state.reshape(rows_local, cols_local, 5, slot_width),
        moved_share.reshape(rows_local, cols_local),
    )


def solution(mesh):
    in_specs = (
        P("gx", "gy", None, None),
        P("gx", "gy", None),
        P("gx", "gy", None),
        P("gx", "gy"),
        P("gx", "gy", None),
        P("gx", "gy"),
    )
    out_specs = (P("gx", "gy", None, None), P("gx", "gy"))
    return jax.shard_map(body, mesh=mesh, in_specs=in_specs, out_specs=out_specs, check_vma=False)
```

```python
import functools
import math

import jax
import jax.numpy as jnp
from jax import lax
from jax.experimental import pallas as pl
from jax.experimental.pallas import tpu as pltpu
from jax.sharding import PartitionSpec as P

OFFSETS = tuple((a, b) for a in (-1, 0, 1) for b in (-1, 0, 1) if (a, b) != (0, 0))
UNROLL = 4


def extended(block, sides, width):
    for axis, dim in sides:
        count = lax.axis_size(axis)
        forward = [(i, i + 1) for i in range(count - 1)]
        forward.append((count - 1, 0))
        backward = [(target, source) for source, target in forward]
        low = lax.ppermute(
            lax.slice_in_dim(block, block.shape[dim] - width, None, axis=dim), axis, forward
        )
        high = lax.ppermute(lax.slice_in_dim(block, 0, width, axis=dim), axis, backward)
        block = jnp.concatenate([low, block, high], axis=dim)
    return block


def split3(value):
    high = value.astype(jnp.bfloat16).astype(jnp.float32)
    rest = value - high
    mid = rest.astype(jnp.bfloat16).astype(jnp.float32)
    return high, mid, rest - mid


def density_kernel(
    rows, cols, pair_ref, send_ref, halo_ref, smooth_ref,
    out_ref, lhs_ref, mass_ref, own_ref, sq_ref, acc_ref, list_ref
):
    tiles = rows * cols
    width = smooth_ref.shape[1]
    wide = cols + 2
    sources = (rows + 2) * wide
    row = lax.broadcasted_iota(jnp.int32, (8, width), 0)

    def spread(ref, tile, index):
        return jnp.broadcast_to(ref[tile, index : index + 1, :], (8, width))

    def centre(t):
        tx = t // cols
        return (tx + 1) * wide + (t - tx * cols) + 1

    def point(tile):
        x = spread(halo_ref, tile, 0) - 0.5
        y = spread(halo_ref, tile, 1) - 0.5
        z = spread(halo_ref, tile, 2) - 0.5
        return x, y, z, x * x + y * y + z * z

    def prep(s, ptr):
        x, y, z, norm_sq = point(s)
        root = spread(halo_ref, s, 3)
        feat = jnp.where(row == 0, x, jnp.where(row == 1, y, jnp.where(row == 2, z, 0.0)))
        feat = jnp.where(row == 3, norm_sq, jnp.where(row == 4, 1.0, feat)) * (root * root)
        high, mid, low = split3(feat)
        turned = jnp.concatenate([high, high, mid, mid, high, low, root], axis=0).T
        lhs_ref[s] = turned[:, :48].astype(jnp.bfloat16)
        mass = jnp.broadcast_to(turned[:, 48:49], (width, width))
        mass_ref[s, 0] = mass
        mass_ref[s, 1] = mass + mass

        t = jnp.minimum(s, tiles - 1)
        base = centre(t)
        x, y, z, norm_sq = point(base)
        h = jnp.broadcast_to(smooth_ref[pl.ds(t, 1), :], (8, width))
        inv = 1.0 / (h * h)
        plain = jnp.where(row == 0, x, jnp.where(row == 1, y, z)) * -2.0
        plain = jnp.where(row < 3, plain, jnp.where(row == 3, 1.0, norm_sq))
        own_ref[t, 0] = jnp.where(row < 5, plain * inv, 0.0)
        own_ref[t, 1] = jnp.where(row == 0, 2.0, jnp.where(row == 4, -2.0 * x, 0.0)) * inv
        own_ref[t, 2] = jnp.where(row == 1, 2.0, jnp.where(row == 4, -2.0 * y, 0.0)) * inv
        own_ref[t, 3] = jnp.where(row == 4, inv, 0.0)
        middle = (base << 16) | (t << 4) | 5
        list_ref[ptr] = middle
        end = ptr + 1
        for k, (a, b) in enumerate(OFFSETS):
            list_ref[end] = middle + ((a * wide + b) * 65536 + a * 4 + b)
            end = end + pair_ref[t * 8 + k]
        return jnp.where(s < tiles, end, ptr)

    total = lax.fori_loop(0, sources, prep, jnp.int32(0), unroll=4 if sources % 4 == 0 else 1)
    for u in range(3 * UNROLL):
        list_ref[total + u] = (sources << 16) | 5
    lhs_ref[sources] = jnp.zeros((width, 48), jnp.bfloat16)
    mass_ref[sources] = jnp.zeros((2, width, width), jnp.float32)
    acc_ref[...] = jnp.zeros_like(acc_ref)
    out_ref[...] = jnp.zeros_like(out_ref)

    def products(first, slot):
        for u in range(UNROLL):
            entry = list_ref[first + u]
            t = (entry >> 4) & 4095
            off_x = (((entry >> 2) & 3) - 1).astype(jnp.float32)
            off_y = ((entry & 3) - 1).astype(jnp.float32)
            off_sq = off_x * off_x + off_y * off_y
            form = own_ref[t, 0] + off_x * own_ref[t, 1] + off_y * own_ref[t, 2] + off_sq * own_ref[t, 3]
            high, mid, low = split3(form)
            rhs = jnp.concatenate([high, mid, high, mid, low, high], axis=0).astype(jnp.bfloat16)
            sq_ref[slot, u] = jnp.dot(
                lhs_ref[entry >> 16], rhs, preferred_element_type=jnp.float32
            )

    def sums(first, slot):
        for u in range(UNROLL):
            entry = list_ref[first + u]
            source = entry >> 16
            t = (entry >> 4) & 4095
            outer_sum = jnp.zeros((8, width), jnp.float32)
            inner_sum = jnp.zeros((8, width), jnp.float32)
            for g in range(width // 8):
                at = pl.ds(8 * g, 8)
                sq = jnp.maximum(sq_ref[slot, u, at, :], 1e-20)
                ratio = sq * lax.rsqrt(sq)
                outer = jnp.maximum(mass_ref[source, 1, at, :] - ratio, 0.0)
                inner = jnp.maximum(mass_ref[source, 0, at, :] - ratio, 0.0)
                outer_sum = outer_sum + outer * outer * outer
                inner_sum = inner_sum + inner * inner * inner
            acc_ref[t] += outer_sum - 4.0 * inner_sum

    products(0, 0)

    def step(i, carry):
        first = i * (2 * UNROLL)
        products(first + UNROLL, 1)
        sums(first, 0)
        products(first + 2 * UNROLL, 0)
        sums(first + UNROLL, 1)
        return carry

    lax.fori_loop(0, (total + 2 * UNROLL - 1) // (2 * UNROLL), step, 0)

    def finish(t, carry):
        summed = jnp.sum(acc_ref[t], axis=0, keepdims=True)
        h = smooth_ref[pl.ds(t, 1), :]
        norm = 0.25 / (math.pi * h * h * h)
        alive = halo_ref[centre(t), 3:4, :] > 0.0
        out_ref[pl.ds(send_ref[t], 1), :] = jnp.where(alive, summed * norm, 0.0)
        return carry

    lax.fori_loop(0, tiles, finish, 0, unroll=4)


def place_kernel(tiles, from_ref, state_ref, dens_ref, out_ref):
    def put(s, carry):
        row = from_ref[s]
        out_ref[s, 0:4, :] = state_ref[row, 0:4, :]
        out_ref[s, 4:5, :] = dens_ref[pl.ds(row, 1), :]
        return carry

    lax.fori_loop(0, tiles, put, 0, unroll=8)


SMEM = pl.BlockSpec(memory_space=pltpu.SMEM)
VMEM = pl.BlockSpec(memory_space=pltpu.VMEM)


def body(positions, masses, smoothing, counts, pair_list, dest):
    rows_local, cols_local = counts.shape
    slot_width = masses.shape[2]
    grid_x = lax.axis_size("gx")
    grid_y = lax.axis_size("gy")
    device_total = grid_x * grid_y
    tile_total = rows_local * cols_local
    capacity = max(2, 2 * tile_total // device_total)
    send_rows = device_total * capacity
    slot_ids = jnp.arange(slot_width, dtype=jnp.int32)
    valid_slot = slot_ids[None, None, :] < counts[:, :, None]
    masked = jnp.where(valid_slot, masses, jnp.zeros_like(masses))
    packed = jnp.concatenate([positions, masked[:, :, None, :]], axis=2)
    root = jnp.where(valid_slot, jnp.cbrt(masses), jnp.zeros_like(masses))
    rooted = jnp.concatenate([positions, root[:, :, None, :]], axis=2)
    padded = extended(rooted, (("gx", 0), ("gy", 1)), 1)
    weights = pair_list.astype(jnp.float32)

    row_span = cols_local * grid_y
    slot_x = dest // row_span
    slot_y = dest % row_span
    target = (slot_x // rows_local * grid_y + slot_y // cols_local).reshape(-1)
    slot_local = (slot_x % rows_local * cols_local + slot_y % cols_local).reshape(-1)
    tile_order = jnp.arange(tile_total, dtype=jnp.int32)
    same_target = target[:, None] == target[None, :]
    earlier = tile_order[None, :] < tile_order[:, None]
    rank_slot = jnp.sum(jnp.logical_and(same_target, earlier).astype(jnp.int32), axis=1)
    send_index = target * capacity + rank_slot

    tile_count = counts.astype(jnp.float32)
    padded_count = jnp.sum((padded[:, :, 3, :] > 0.0).astype(jnp.float32), axis=-1)
    neighbour_sum = jnp.zeros((rows_local, cols_local), jnp.float32)
    for k, (a, b) in enumerate(OFFSETS):
        beside = padded_count[1 + a : 1 + a + rows_local, 1 + b : 1 + b + cols_local]
        neighbour_sum = neighbour_sum + weights[:, :, k] * beside
    pair_work = tile_count * (tile_count + neighbour_sum)
    local_work = jnp.sum(pair_work)

    lane = slot_ids[None, :]
    note = jnp.where(lane == 0, pair_work.reshape(-1, 1), 0.0)
    note = jnp.where(lane == 1, (slot_local + 1).astype(jnp.float32)[:, None], note)
    tile_state = jnp.concatenate(
        [packed.reshape(tile_total, 4, slot_width), note[:, None, :]], axis=1
    )
    send_state = jnp.zeros((send_rows, 5, slot_width), jnp.float32).at[send_index].set(tile_state)
    mark = jnp.logical_and(jnp.arange(5)[:, None] == 4, lane == 2)
    send_state = jnp.where(mark[None], local_work, send_state)
    recv_state = lax.all_to_all(
        send_state.reshape(device_total, capacity, 5, slot_width),
        ("gx", "gy"),
        split_axis=0,
        concat_axis=0,
        tiled=True,
    ).reshape(send_rows, 5, slot_width)

    sources = (rows_local + 2) * (cols_local + 2)
    send_density = pl.pallas_call(
        functools.partial(density_kernel, rows_local, cols_local),
        out_shape=jax.ShapeDtypeStruct((send_rows, slot_width), jnp.float32),
        in_specs=[SMEM, SMEM, VMEM, VMEM],
        out_specs=VMEM,
        scratch_shapes=[
            pltpu.VMEM((sources + 1, slot_width, 48), jnp.bfloat16),
            pltpu.VMEM((sources + 1, 2, slot_width, slot_width), jnp.float32),
            pltpu.VMEM((tile_total, 4, 8, slot_width), jnp.float32),
            pltpu.VMEM((2, UNROLL, slot_width, slot_width), jnp.float32),
            pltpu.VMEM((tile_total, 8, slot_width), jnp.float32),
            pltpu.SMEM((9 * tile_total + 4 * UNROLL,), jnp.int32),
        ],
        compiler_params=pltpu.CompilerParams(vmem_limit_bytes=52 * 1024 * 1024),
        cost_estimate=pl.CostEstimate(
            flops=20 * 9 * tile_total * slot_width * slot_width,
            bytes_accessed=180 * 2**20,
            transcendentals=9 * tile_total * slot_width * slot_width,
        ),
        name="density",
    )(
        pair_list.reshape(-1),
        send_index,
        padded.reshape(sources, 4, slot_width),
        smoothing.reshape(tile_total, slot_width),
    )

    recv_density = lax.all_to_all(
        send_density.reshape(device_total, capacity, slot_width),
        ("gx", "gy"),
        split_axis=0,
        concat_axis=0,
        tiled=True,
    ).reshape(send_rows, slot_width)

    recv_note = recv_state[:, 4, :3]
    recv_slot = recv_note[:, 1].astype(jnp.int32) - 1
    hit = recv_slot[None, :] == tile_order[:, None]
    recv_order = jnp.arange(send_rows, dtype=jnp.int32)
    from_row = jnp.sum(jnp.where(hit, recv_order[None, :], 0), axis=1)
    total_work = jnp.sum(recv_note.reshape(device_total, capacity, 3)[:, 0, 2])
    moved_work = jnp.sum(jnp.where(hit, recv_note[:, 0][None, :], 0.0), axis=1)
    moved_share = moved_work * float(tile_total * device_total) / total_work

    moved_state = pl.pallas_call(
        functools.partial(place_kernel, tile_total),
        out_shape=jax.ShapeDtypeStruct((tile_total, 5, slot_width), jnp.float32),
        in_specs=[SMEM, VMEM, VMEM],
        out_specs=VMEM,
        name="place",
    )(from_row, recv_state, recv_density)
    return (
        moved_state.reshape(rows_local, cols_local, 5, slot_width),
        moved_share.reshape(rows_local, cols_local),
    )


def solution(mesh):
    in_specs = (
        P("gx", "gy", None, None),
        P("gx", "gy", None),
        P("gx", "gy", None),
        P("gx", "gy"),
        P("gx", "gy", None),
        P("gx", "gy"),
    )
    out_specs = (P("gx", "gy", None, None), P("gx", "gy"))
    return jax.shard_map(body, mesh=mesh, in_specs=in_specs, out_specs=out_specs, check_vma=False)
```

```python
import functools
import math

import jax
import jax.numpy as jnp
from jax import lax
from jax.experimental import pallas as pl
from jax.experimental.pallas import tpu as pltpu
from jax.sharding import PartitionSpec as P

OFFSETS = tuple((a, b) for a in (-1, 0, 1) for b in (-1, 0, 1) if (a, b) != (0, 0))
UNROLL = 4


def extended(block, sides, width):
    for axis, dim in sides:
        count = lax.axis_size(axis)
        forward = [(i, i + 1) for i in range(count - 1)]
        forward.append((count - 1, 0))
        backward = [(target, source) for source, target in forward]
        low = lax.ppermute(
            lax.slice_in_dim(block, block.shape[dim] - width, None, axis=dim), axis, forward
        )
        high = lax.ppermute(lax.slice_in_dim(block, 0, width, axis=dim), axis, backward)
        block = jnp.concatenate([low, block, high], axis=dim)
    return block


def split3(value):
    high = value.astype(jnp.bfloat16).astype(jnp.float32)
    rest = value - high
    mid = rest.astype(jnp.bfloat16).astype(jnp.float32)
    return high, mid, rest - mid


def density_kernel(
    rows, cols, pair_ref, send_ref, halo_ref, smooth_ref,
    out_ref, lhs_ref, mass_ref, own_ref, sq_ref, acc_ref, list_ref
):
    tiles = rows * cols
    width = smooth_ref.shape[1]
    wide = cols + 2
    sources = (rows + 2) * wide
    row = lax.broadcasted_iota(jnp.int32, (8, width), 0)

    def spread(ref, tile, index):
        return jnp.broadcast_to(ref[tile, index : index + 1, :], (8, width))

    def centre(t):
        tx = t // cols
        return (tx + 1) * wide + (t - tx * cols) + 1

    def point(tile):
        x = spread(halo_ref, tile, 0) - 0.5
        y = spread(halo_ref, tile, 1) - 0.5
        z = spread(halo_ref, tile, 2) - 0.5
        return x, y, z, x * x + y * y + z * z

    def prep(s, ptr):
        x, y, z, norm_sq = point(s)
        root = spread(halo_ref, s, 3)
        feat = jnp.where(row == 0, x, jnp.where(row == 1, y, jnp.where(row == 2, z, 0.0)))
        feat = jnp.where(row == 3, norm_sq, jnp.where(row == 4, 1.0, feat)) * (root * root)
        high, mid, low = split3(feat)
        turned = jnp.concatenate([high, high, mid, mid, high, low, root], axis=0).T
        lhs_ref[s] = turned[:, :48].astype(jnp.bfloat16)
        mass = jnp.broadcast_to(turned[:, 48:49], (width, width))
        mass_ref[s, 0] = mass
        mass_ref[s, 1] = mass + mass

        t = jnp.minimum(s, tiles - 1)
        base = centre(t)
        x, y, z, norm_sq = point(base)
        h = jnp.broadcast_to(smooth_ref[pl.ds(t, 1), :], (8, width))
        inv = 1.0 / (h * h)
        plain = jnp.where(row == 0, x, jnp.where(row == 1, y, z)) * -2.0
        plain = jnp.where(row < 3, plain, jnp.where(row == 3, 1.0, norm_sq))
        own_ref[t, 0] = jnp.where(row < 5, plain * inv, 0.0)
        own_ref[t, 1] = jnp.where(row == 0, 2.0, jnp.where(row == 4, -2.0 * x, 0.0)) * inv
        own_ref[t, 2] = jnp.where(row == 1, 2.0, jnp.where(row == 4, -2.0 * y, 0.0)) * inv
        own_ref[t, 3] = jnp.where(row == 4, inv, 0.0)
        middle = (base << 16) | (t << 4) | 5
        list_ref[ptr] = middle
        end = ptr + 1
        for k, (a, b) in enumerate(OFFSETS):
            list_ref[end] = middle + ((a * wide + b) * 65536 + a * 4 + b)
            end = end + pair_ref[t * 8 + k]
        return jnp.where(s < tiles, end, ptr)

    total = lax.fori_loop(0, sources, prep, jnp.int32(0), unroll=4 if sources % 4 == 0 else 1)
    for u in range(3 * UNROLL):
        list_ref[total + u] = (sources << 16) | 5
    lhs_ref[sources] = jnp.zeros((width, 48), jnp.bfloat16)
    mass_ref[sources] = jnp.zeros((2, width, width), jnp.float32)
    acc_ref[...] = jnp.zeros_like(acc_ref)
    out_ref[...] = jnp.zeros_like(out_ref)

    def products(first, slot):
        for u in range(UNROLL):
            entry = list_ref[first + u]
            t = (entry >> 4) & 4095
            off_x = (((entry >> 2) & 3) - 1).astype(jnp.float32)
            off_y = ((entry & 3) - 1).astype(jnp.float32)
            off_sq = off_x * off_x + off_y * off_y
            form = own_ref[t, 0] + off_x * own_ref[t, 1] + off_y * own_ref[t, 2] + off_sq * own_ref[t, 3]
            high, mid, low = split3(form)
            rhs = jnp.concatenate([high, mid, high, mid, low, high], axis=0).astype(jnp.bfloat16)
            sq_ref[slot, u] = jnp.dot(
                lhs_ref[entry >> 16], rhs, preferred_element_type=jnp.float32
            )

    def sums(first, slot):
        for u in range(UNROLL):
            entry = list_ref[first + u]
            source = entry >> 16
            t = (entry >> 4) & 4095
            outer_sum = jnp.zeros((8, width), jnp.float32)
            inner_sum = jnp.zeros((8, width), jnp.float32)
            for g in range(width // 8):
                at = pl.ds(8 * g, 8)
                sq = jnp.maximum(sq_ref[slot, u, at, :], 1e-20)
                ratio = sq * lax.rsqrt(sq)
                outer = jnp.maximum(mass_ref[source, 1, at, :] - ratio, 0.0)
                inner = jnp.maximum(mass_ref[source, 0, at, :] - ratio, 0.0)
                outer_sum = outer_sum + outer * outer * outer
                inner_sum = inner_sum + inner * inner * inner
            acc_ref[t] += outer_sum - 4.0 * inner_sum

    products(0, 0)

    def step(i, carry):
        first = i * (2 * UNROLL)
        products(first + UNROLL, 1)
        sums(first, 0)
        products(first + 2 * UNROLL, 0)
        sums(first + UNROLL, 1)
        return carry

    lax.fori_loop(0, (total + 2 * UNROLL - 1) // (2 * UNROLL), step, 0)

    def finish(t, carry):
        summed = jnp.sum(acc_ref[t], axis=0, keepdims=True)
        h = smooth_ref[pl.ds(t, 1), :]
        norm = 0.25 / (math.pi * h * h * h)
        alive = halo_ref[centre(t), 3:4, :] > 0.0
        out_ref[pl.ds(send_ref[t], 1), :] = jnp.where(alive, summed * norm, 0.0)
        return carry

    lax.fori_loop(0, tiles, finish, 0, unroll=4)


def pack_kernel(tiles, send_ref, packed_ref, note_ref, out_ref):
    lane = lax.broadcasted_iota(jnp.int32, (1, note_ref.shape[1]), 1)
    blank = jnp.where(lane == 2, note_ref[0:1, :], 0.0)
    out_ref[...] = jnp.broadcast_to(blank[None], out_ref.shape)

    def put(t, carry):
        row = send_ref[t]
        out_ref[row, 0:4, :] = packed_ref[t]
        out_ref[row, 4:5, :] = note_ref[pl.ds(t, 1), :]
        return carry

    lax.fori_loop(0, tiles, put, 0, unroll=8)


def place_kernel(tiles, from_ref, state_ref, dens_ref, out_ref):
    def put(s, carry):
        row = from_ref[s]
        out_ref[s, 0:4, :] = state_ref[row, 0:4, :]
        out_ref[s, 4:5, :] = dens_ref[pl.ds(row, 1), :]
        return carry

    lax.fori_loop(0, tiles, put, 0, unroll=8)


SMEM = pl.BlockSpec(memory_space=pltpu.SMEM)
VMEM = pl.BlockSpec(memory_space=pltpu.VMEM)


def body(positions, masses, smoothing, counts, pair_list, dest):
    rows_local, cols_local = counts.shape
    slot_width = masses.shape[2]
    grid_x = lax.axis_size("gx")
    grid_y = lax.axis_size("gy")
    device_total = grid_x * grid_y
    tile_total = rows_local * cols_local
    capacity = max(2, 2 * tile_total // device_total)
    send_rows = device_total * capacity
    slot_ids = jnp.arange(slot_width, dtype=jnp.int32)
    valid_slot = slot_ids[None, None, :] < counts[:, :, None]
    masked = jnp.where(valid_slot, masses, jnp.zeros_like(masses))
    packed = jnp.concatenate([positions, masked[:, :, None, :]], axis=2)
    root = jnp.where(valid_slot, jnp.cbrt(masses), jnp.zeros_like(masses))
    rooted = jnp.concatenate([positions, root[:, :, None, :]], axis=2)
    padded = extended(rooted, (("gx", 0), ("gy", 1)), 1)
    weights = pair_list.astype(jnp.float32)

    row_span = cols_local * grid_y
    slot_x = dest // row_span
    slot_y = dest % row_span
    target = (slot_x // rows_local * grid_y + slot_y // cols_local).reshape(-1)
    slot_local = (slot_x % rows_local * cols_local + slot_y % cols_local).reshape(-1)
    tile_order = jnp.arange(tile_total, dtype=jnp.int32)
    same_target = target[:, None] == target[None, :]
    earlier = tile_order[None, :] < tile_order[:, None]
    rank_slot = jnp.sum(jnp.logical_and(same_target, earlier).astype(jnp.int32), axis=1)
    send_index = target * capacity + rank_slot

    tile_count = counts.astype(jnp.float32)
    padded_count = jnp.sum((padded[:, :, 3, :] > 0.0).astype(jnp.float32), axis=-1)
    neighbour_sum = jnp.zeros((rows_local, cols_local), jnp.float32)
    for k, (a, b) in enumerate(OFFSETS):
        beside = padded_count[1 + a : 1 + a + rows_local, 1 + b : 1 + b + cols_local]
        neighbour_sum = neighbour_sum + weights[:, :, k] * beside
    pair_work = tile_count * (tile_count + neighbour_sum)
    local_work = jnp.sum(pair_work)

    lane = slot_ids[None, :]
    note = jnp.where(lane == 0, pair_work.reshape(-1, 1), 0.0)
    note = jnp.where(lane == 1, (slot_local + 1).astype(jnp.float32)[:, None], note)
    note = jnp.where(lane == 2, local_work, note)
    send_state = pl.pallas_call(
        functools.partial(pack_kernel, tile_total),
        out_shape=jax.ShapeDtypeStruct((send_rows, 5, slot_width), jnp.float32),
        in_specs=[SMEM, VMEM, VMEM],
        out_specs=VMEM,
        name="pack",
    )(send_index, packed.reshape(tile_total, 4, slot_width), note)
    recv_state = lax.all_to_all(
        send_state.reshape(device_total, capacity, 5, slot_width),
        ("gx", "gy"),
        split_axis=0,
        concat_axis=0,
        tiled=True,
    ).reshape(send_rows, 5, slot_width)

    sources = (rows_local + 2) * (cols_local + 2)
    send_density = pl.pallas_call(
        functools.partial(density_kernel, rows_local, cols_local),
        out_shape=jax.ShapeDtypeStruct((send_rows, slot_width), jnp.float32),
        in_specs=[SMEM, SMEM, VMEM, VMEM],
        out_specs=VMEM,
        scratch_shapes=[
            pltpu.VMEM((sources + 1, slot_width, 48), jnp.bfloat16),
            pltpu.VMEM((sources + 1, 2, slot_width, slot_width), jnp.float32),
            pltpu.VMEM((tile_total, 4, 8, slot_width), jnp.float32),
            pltpu.VMEM((2, UNROLL, slot_width, slot_width), jnp.float32),
            pltpu.VMEM((tile_total, 8, slot_width), jnp.float32),
            pltpu.SMEM((9 * tile_total + 4 * UNROLL,), jnp.int32),
        ],
        compiler_params=pltpu.CompilerParams(vmem_limit_bytes=52 * 1024 * 1024),
        cost_estimate=pl.CostEstimate(
            flops=20 * 9 * tile_total * slot_width * slot_width,
            bytes_accessed=180 * 2**20,
            transcendentals=9 * tile_total * slot_width * slot_width,
        ),
        name="density",
    )(
        pair_list.reshape(-1),
        send_index,
        padded.reshape(sources, 4, slot_width),
        smoothing.reshape(tile_total, slot_width),
    )

    recv_density = lax.all_to_all(
        send_density.reshape(device_total, capacity, slot_width),
        ("gx", "gy"),
        split_axis=0,
        concat_axis=0,
        tiled=True,
    ).reshape(send_rows, slot_width)

    recv_note = recv_state[:, 4, :3]
    recv_slot = recv_note[:, 1].astype(jnp.int32) - 1
    hit = recv_slot[None, :] == tile_order[:, None]
    recv_order = jnp.arange(send_rows, dtype=jnp.int32)
    from_row = jnp.sum(jnp.where(hit, recv_order[None, :], 0), axis=1)
    total_work = jnp.sum(recv_note.reshape(device_total, capacity, 3)[:, 0, 2])
    moved_work = jnp.sum(jnp.where(hit, recv_note[:, 0][None, :], 0.0), axis=1)
    moved_share = moved_work * float(tile_total * device_total) / total_work

    moved_state = pl.pallas_call(
        functools.partial(place_kernel, tile_total),
        out_shape=jax.ShapeDtypeStruct((tile_total, 5, slot_width), jnp.float32),
        in_specs=[SMEM, VMEM, VMEM],
        out_specs=VMEM,
        name="place",
    )(from_row, recv_state, recv_density)
    return (
        moved_state.reshape(rows_local, cols_local, 5, slot_width),
        moved_share.reshape(rows_local, cols_local),
    )


def solution(mesh):
    in_specs = (
        P("gx", "gy", None, None),
        P("gx", "gy", None),
        P("gx", "gy", None),
        P("gx", "gy"),
        P("gx", "gy", None),
        P("gx", "gy"),
    )
    out_specs = (P("gx", "gy", None, None), P("gx", "gy"))
    return jax.shard_map(body, mesh=mesh, in_specs=in_specs, out_specs=out_specs, check_vma=False)
```
